256 devices in a mesh: groups: 2 (over z), adapter: 16 (over x, core), tensor: 8 (over y).
Axes of the slice: x: 8, y: 8, z: 2, core: 2. Of those that a mesh axis runs over, the one named last changes fastest.
The devices are a block of a 8x8x16 slice.
Arguments:
- tokens: bfloat16 [8192, 8192], P(('groups', 'adapter'), 'tensor'), parts along dimension 0, may hold values from -6 to 6
- query_weight: bfloat16 [8192, 8192], P('tensor', 'adapter'), may hold values from -0.0625 to 0.0625
- adapter_down_weight: bfloat16 [512, 16, 8192], P('adapter', None, 'tensor'), may hold values from -0.0625 to 0.0625
- adapter_up_weight: bfloat16 [512, 16, 8192], P('adapter'), may hold values from -1.5 to 1.5
- block_adapter_ids: int32 [64], P('groups'), parts along dimension 0, may hold values from 0 to 511, as said below
- block_live_count: int32 [64], P('groups'), parts along dimension 0, may hold values from 1 to 128
- adapter_slot_index: int32 [1024], P('groups'), parts along dimension 0, may hold values from 0 to 511, as said below
Outputs:
- query: bfloat16 [8192, 8192], P(('groups', 'tensor'), 'adapter'), parts along dimension 0
The draws below stay inside these ranges and needn't reach their ends.
There are 2 independent parts, one for each index of `groups`. The reference program is written for one: setup_inputs(seed, part) draws one part's arguments, and reference() takes and returns one part's arrays. A program takes and returns all parts, laid end to end along the dimension named above; an argument that names none is the same for every part. Nothing has to cross between parts.
Inputs may be any that keep to these rules, and one draw needn't show every extreme that they name: Counting blocks by the owner range adapter_slot_index[block_adapter_ids[k]] // 32, no owner has more than 4 blocks, and one owner has exactly 4 in every draw. `adapter_slot_index`: A permutation: each slot holds exactly one adapter.
All inputs are finite; a program needn't handle non-finite values.
Results may differ from the reference program's by a relative error of at most 0.014.
Values may be sent and summed in bfloat16 or wider, within the bound.
No kernel may reach another device: no remote copies, remote signals or barrier semaphores. Data moves between devices by JAX's collectives and lax.ppermute only.
A program may use at most 128 MiB of HBM per device.

```python
import jax
import jax.numpy as jnp

MODEL_WIDTH = 8192
QUERY_OUTPUTS = 8192
ADAPTER_RANK = 16
ADP_DEV = 32
BLOCK = 128
ADAPTER_COUNT = 512
FEAT = 1024
CAP = 4
BLOCKS = 32
TOKENS = 4096


def plan_draw(key):
    owner_count = ADAPTER_COUNT // ADP_DEV
    slot_table = jax.random.permutation(jax.random.fold_in(key, 101), jnp.arange(ADAPTER_COUNT, dtype=jnp.int32)).astype(jnp.int32)
    holder = jnp.argsort(slot_table, stable=True).astype(jnp.int32)
    hottest = jax.random.randint(jax.random.fold_in(key, 102), (), 0, owner_count, dtype=jnp.int32)
    seat_owner = jnp.arange((owner_count - 1) * CAP, dtype=jnp.int32) // CAP
    seat_owner = seat_owner + (seat_owner >= hottest).astype(jnp.int32)
    seat_owner = jax.random.permutation(jax.random.fold_in(key, 103), seat_owner)[:BLOCKS - CAP]
    owner_list = jnp.concatenate([jnp.full((CAP,), hottest, jnp.int32), seat_owner.astype(jnp.int32)])
    owner_list = jax.random.permutation(jax.random.fold_in(key, 104), owner_list)
    local_slot = jax.random.randint(jax.random.fold_in(key, 105), (BLOCKS,), 0, ADP_DEV, dtype=jnp.int32)
    adapters = holder[owner_list * ADP_DEV + local_slot]
    return (slot_table, adapters.astype(jnp.int32))


def draw_block_adapter_ids(key, part):
    return plan_draw(key)[1]


def draw_adapter_slot_index(key, part):
    return plan_draw(key)[0]


def touch_ends(drawn, stream_key, low, top_value):
    longest = drawn.shape.index(max(drawn.shape))
    spots = []
    for shift in (0, 1):
        where = [jax.random.randint(jax.random.fold_in(stream_key, axis), (), 0, length) for axis, length in enumerate(drawn.shape)]
        where[longest] = (where[longest] + shift) % drawn.shape[longest]
        spots.append(tuple(where))
    return drawn.at[spots[0]].set(low).at[spots[1]].set(top_value)


def levels(own_key, dims, cuts, low, largest):
    def one(position, blocks):
        draws = jax.random.uniform(jax.random.fold_in(jax.random.fold_in(own_key, 6), position), (blocks,), jnp.float32, low / len(cuts), largest / len(cuts))
        return jnp.repeat(jnp.exp(draws), dims[position] // blocks).reshape((-1,) + (1,) * (len(dims) - position - 1))

    factor_of = one(*cuts[0])
    for cut in cuts[1:]:
        factor_of = factor_of * one(*cut)
    return factor_of


def normal_values(rng, extent, spread, reach, pieces=(), held_as=jnp.bfloat16):
    array = spread * jax.random.normal(rng, extent, jnp.float32)
    if pieces:
        array = array * levels(rng, extent, pieces, -0.22, 0.18)
    return jnp.clip(array, -reach, reach).astype(held_as)


def setup_inputs(seed: int = 0, part: int = 0) -> dict:
    key_list = jax.random.split(jax.random.key(seed), 8)
    own_keys = jax.random.split(jax.random.fold_in(key_list[7], part), 8)
    tokens = normal_values(own_keys[0], (TOKENS, MODEL_WIDTH), 1.0, 6.0, ((0, 16), (1, 8)))
    query_weight = normal_values(key_list[1], (MODEL_WIDTH, QUERY_OUTPUTS), MODEL_WIDTH ** -0.5, 0.0625, ((0, 8), (1, 16)))
    adapter_down_weight = normal_values(key_list[2], (ADAPTER_COUNT, ADAPTER_RANK, MODEL_WIDTH), MODEL_WIDTH ** -0.5, 0.0625, ((0, 16), (2, 8)))
    adapter_up_weight = normal_values(key_list[3], (ADAPTER_COUNT, ADAPTER_RANK, QUERY_OUTPUTS), ADAPTER_RANK ** -0.5, 1.5, ((0, 16),))
    block_adapter_ids = draw_block_adapter_ids(jax.random.fold_in(jax.random.fold_in(key_list[7], part), 71), part)
    block_live_count = touch_ends(jax.random.randint(own_keys[5], (BLOCKS,), 1, BLOCK + 1), jax.random.fold_in(own_keys[5], 1), 1, BLOCK).astype(jnp.int32)
    adapter_slot_index = draw_adapter_slot_index(jax.random.fold_in(jax.random.fold_in(key_list[7], part), 71), part)
    return dict(tokens=tokens, query_weight=query_weight, adapter_down_weight=adapter_down_weight, adapter_up_weight=adapter_up_weight, block_adapter_ids=block_adapter_ids, block_live_count=block_live_count, adapter_slot_index=adapter_slot_index)


def reference(tokens, query_weight, adapter_down_weight, adapter_up_weight, block_adapter_ids, block_live_count, adapter_slot_index):
    block_slot_index = adapter_slot_index[block_adapter_ids].astype(jnp.int32)
    down_weight_blocks = adapter_down_weight[block_slot_index].astype(jnp.float32)
    up_weight_blocks = adapter_up_weight[block_slot_index].astype(jnp.float32)
    positions = jnp.arange(BLOCK, dtype=jnp.int32)
    live_mask = (positions[None, :] < block_live_count[:, None]).astype(jnp.float32)
    token_blocks = tokens.reshape(BLOCKS, BLOCK, MODEL_WIDTH).astype(jnp.float32)
    total = jnp.zeros((TOKENS, QUERY_OUTPUTS), jnp.float32)
    for slice_index in range(MODEL_WIDTH // FEAT):
        low_edge = slice_index * FEAT
        high_edge = low_edge + FEAT
        shrunk = jnp.einsum("ksd,krd->ksr", token_blocks[:, :, low_edge:high_edge], down_weight_blocks[:, :, low_edge:high_edge])
        shrunk = (shrunk * live_mask[:, :, None]).astype(jnp.bfloat16)
        adapter_part = jnp.einsum("ksr,krf->ksf", shrunk.astype(jnp.float32), up_weight_blocks).reshape(TOKENS, QUERY_OUTPUTS)
        base_part = jnp.dot(tokens[:, low_edge:high_edge], query_weight[low_edge:high_edge, :], preferred_element_type=jnp.float32)
        partial_value = (base_part + 2.0 * adapter_part).astype(jnp.bfloat16)
        total = total + partial_value.astype(jnp.float32)
    return total.astype(jnp.bfloat16)
```

```python
import functools

import jax
import jax.numpy as jnp
from jax import lax
from jax.experimental import pallas as pl
from jax.experimental.pallas import tpu as pltpu
from jax.sharding import PartitionSpec as P


BLOCK = 128
CORES = 2
CHUNKS = 1

adapter_scale = 2.0


bf16 = jnp.bfloat16
f32 = jnp.float32
i32 = jnp.int32
VMEM = pl.BlockSpec(memory_space=pltpu.VMEM)
SMEM = pl.BlockSpec(memory_space=pltpu.SMEM)
ANY = pl.BlockSpec(memory_space=pl.ANY)


def shift_chips(v, chips, step):
    pairs = [
        (x * CORES + c, ((x + step) % chips) * CORES + c)
        for x in range(chips)
        for c in range(CORES)
    ]
    return lax.ppermute(v, "adapter", pairs)


def swap_cores(v, chips):
    return lax.ppermute(v, "adapter", [(i, i ^ 1) for i in range(chips * CORES)])


def shift_slices(v, slices, step):
    return lax.ppermute(v, "tensor", [(y, (y + step) % slices) for y in range(slices)])


def shift_slices_swap(v, adapters, slices, step):
    pairs = [
        (a * slices + y, (a ^ 1) * slices + (y + step) % slices)
        for a in range(adapters)
        for y in range(slices)
    ]
    return lax.ppermute(v, ("adapter", "tensor"), pairs)


def plan_kernel(
    owners, slices, seats, where, ids, live, index, down, up,
    table, down_out, up_out, counts, seat_slot, sems
):
    slots = down.shape[0]
    rank = down.shape[1]
    blocks = ids.shape[0]
    a, y = where[0], where[1]
    c = lax.rem(a, CORES)
    for i in range(owners):
        counts[i] = 0
    for s in range(seats):
        seat_slot[s] = 0

    def block(k, _):
        slot = index[ids[k]]
        owner = lax.div(slot, slots)
        local = slot - owner * slots
        seat = jnp.minimum(counts[owner], seats - 1)
        counts[owner] = seat + 1
        table[0, k] = owner
        table[1, k] = seat
        table[2, k] = jnp.where(
            owner == a, seat, jnp.where(lax.div(owner, CORES) == lax.div(a, CORES), seats + seat, -1)
        )
        table[3, k] = live[k]

        @pl.when(owner == a)
        def _():
            seat_slot[seat] = local

        return 0

    lax.fori_loop(0, blocks, block, 0)
    cols = up.shape[2] // owners
    parts = slices // seats
    part = cols // parts
    copies = []
    for s in range(seats):
        copies.append(
            pltpu.make_async_copy(
                down.at[seat_slot[s]], down_out.at[pl.ds(s * rank, rank)], sems.at[s]
            )
        )
    up_slot = seat_slot[lax.div(y, parts)]
    low = lax.rem(y, parts) * part
    for d in range(owners):
        copies.append(
            pltpu.make_async_copy(
                up.at[up_slot, :, pl.ds(pl.multiple_of(d * cols + low, part), part)],
                up_out.at[d],
                sems.at[seats + d],
            )
        )
    for copy in copies:
        copy.start()
    for copy in copies:
        copy.wait()


def pick_kernel(rank, blk_dev, table, c_ref, shr, out):
    chips, _, _ = shr.shape
    lane = lax.broadcasted_iota(i32, (rank, BLOCK), 1)
    c = c_ref[0]
    for src in range(chips):
        for j in range(blk_dev):
            k = (src * CORES + c) * blk_dev + j
            seat = table[2, k]
            at = pl.multiple_of(jnp.maximum(seat, 0) * rank, rank)
            v = shr[src, pl.ds(at, rank), j * BLOCK : (j + 1) * BLOCK]
            live = jnp.where(seat < 0, 0, table[3, k])
            v = jnp.where(lane < live, v.astype(f32), 0.0)
            out[src, :, j * BLOCK : (j + 1) * BLOCK] = v.astype(bf16)


def extra_kernel(blk_dev, table, shr, up, y_ref, out):
    owners, rank, rows = shr.shape
    _, blk_chip, _, part = up.shape
    cols = out.shape[1]
    parts = cols // part
    y = y_ref[0]
    total = [jnp.zeros((rank, rows), f32) for _ in range(CORES)]
    for o in range(owners):
        total[o % CORES] = total[o % CORES] + shr[o].astype(f32)
    for b in range(blk_chip):
        j = b % blk_dev
        s = total[b // blk_dev][:, j * BLOCK : (j + 1) * BLOCK].astype(bf16)
        seat = table[1, y * blk_chip + b]
        for h in range(parts):
            u = up[seat * parts + h, b]
            e = lax.dot_general(s, u, (((0,), (0,)), ((), ())), preferred_element_type=f32)
            out[b * BLOCK : (b + 1) * BLOCK, h * part : (h + 1) * part] = adapter_scale * e


def finish_kernel(chunks, *refs):
    c_ref, extra = refs[0], refs[1]
    out = refs[-1]
    n = refs[2].shape[0]
    rows = n * chunks
    c = c_ref[0]
    for q in range(chunks):
        own, dn_own, up_own, oth, dn_oth, up_oth = refs[2 + 6 * q : 8 + 6 * q]
        at = pl.multiple_of(c * rows + q * n, n)
        v = own[...].astype(f32) + dn_own[...].astype(f32) + up_own[...].astype(f32)
        out[pl.ds(at, n)] = (v + extra[pl.ds(at, n)]).astype(bf16)
        at = pl.multiple_of((1 - c) * rows + q * n, n)
        v = oth[...].astype(f32) + dn_oth[...].astype(f32) + up_oth[...].astype(f32)
        out[pl.ds(at, n)] = (v + extra[pl.ds(at, n)]).astype(bf16)


def on_device(
    tokens,
    query_weight,
    adapter_down_weight,
    adapter_up_weight,
    block_adapter_ids,
    block_live_count,
    adapter_slot_index,
):
    owners = lax.axis_size("adapter")
    slices = lax.axis_size("tensor")
    chips = owners // CORES
    half = chips // 2
    a = lax.axis_index("adapter")
    y = lax.axis_index("tensor")
    x, c = a // CORES, a % CORES
    rows, feats = tokens.shape
    cols = query_weight.shape[1]
    _, rank, _ = adapter_up_weight.shape
    blocks = block_adapter_ids.shape[0]
    seats = 2 * blocks // owners
    blk_dev = blocks // owners
    blk_chip = blk_dev * CORES
    parts = slices // seats
    part = cols // parts
    n = rows // CHUNKS

    chunks = [tokens[q * n : (q + 1) * n] for q in range(CHUNKS)]
    ups, dns = [], []
    for q in range(CHUNKS):
        ups.append([shift_chips(chunks[q], chips, 1)])
        dns.append([shift_chips(chunks[q], chips, -1)])
    w_oth = swap_cores(query_weight, chips)
    w_both = jnp.concatenate([query_weight, w_oth], axis=1)

    table, down_own, up_part = pl.pallas_call(
        functools.partial(plan_kernel, owners, slices, seats),
        out_shape=(
            jax.ShapeDtypeStruct((4, blocks), i32),
            jax.ShapeDtypeStruct((seats * rank, feats), bf16),
            jax.ShapeDtypeStruct((owners, rank, part), bf16),
        ),
        in_specs=[SMEM] * 4 + [ANY] * 2,
        out_specs=(SMEM, VMEM, VMEM),
        scratch_shapes=[
            pltpu.SMEM((owners,), i32),
            pltpu.SMEM((seats,), i32),
            pltpu.SemaphoreType.DMA((seats + owners,)),
        ],
        cost_estimate=pl.CostEstimate(flops=10**7, bytes_accessed=10**6, transcendentals=0),
    )(
        jnp.stack([a, y]),
        block_adapter_ids,
        block_live_count,
        adapter_slot_index,
        adapter_down_weight,
        adapter_up_weight,
    )
    down_oth = swap_cores(down_own, chips)
    down_chip = jnp.concatenate([down_own, down_oth], axis=0)
    up_part = lax.all_to_all(up_part, "adapter", 0, 0, tiled=True)
    up_all = jnp.take(up_part, table[0], axis=0)
    up_all = lax.all_to_all(
        up_all.reshape(slices, blk_chip, rank, part), "tensor", 0, 0, tiled=True
    )

    shr_buf = jnp.zeros((chips, CORES * seats * rank, rows), bf16)
    bufs = []

    def put(q, tok, d):
        nonlocal shr_buf
        src = (x + d) % chips
        p = jnp.dot(tok, w_both, preferred_element_type=f32).astype(bf16)
        bufs[q] = lax.dynamic_update_slice(bufs[q], p[None], (src, 0, 0))
        s = lax.dot_general(
            down_chip, tok, (((1,), (1,)), ((), ())), preferred_element_type=f32
        ).astype(bf16)
        shr_buf = lax.dynamic_update_slice(shr_buf, s[None], (src, 0, q * n))

    for q in range(CHUNKS):
        bufs.append(jnp.zeros((chips, n, CORES * cols), bf16))
        put(q, chunks[q], 0)
    for h in range(1, half + 1):
        for q in range(CHUNKS):
            if h == half:
                tok = jnp.concatenate([ups[q][-1], dns[q][-1]], axis=0)
                put(q, tok, half)
                continue
            put(q, ups[q][-1], -h)
            put(q, dns[q][-1], h)
            up, dn = ups[q][-1], dns[q][-1]
            if h == half - 1:
                up, dn = up[: n // 2], dn[n // 2 :]
            ups[q].append(shift_chips(up, chips, 1))
            dns[q].append(shift_chips(dn, chips, -1))

    shr = pl.pallas_call(
        functools.partial(pick_kernel, rank, blk_dev),
        out_shape=jax.ShapeDtypeStruct((chips, rank, rows), bf16),
        in_specs=[SMEM, SMEM, VMEM],
        out_specs=VMEM,
        cost_estimate=pl.CostEstimate(flops=10**7, bytes_accessed=10**6, transcendentals=0),
    )(table, c[None], shr_buf)
    shr, up_all = lax.optimization_barrier((shr, up_all))
    shr = lax.all_to_all(shr, "tensor", 0, 0, tiled=True)
    shr = jnp.sum(shr.astype(f32), axis=0).astype(bf16)
    shr = jnp.broadcast_to(shr[None], (owners, rank, rows))
    shr = lax.all_to_all(shr, "adapter", 0, 0, tiled=True)
    extra = pl.pallas_call(
        functools.partial(extra_kernel, blk_dev),
        out_shape=jax.ShapeDtypeStruct((blk_chip * BLOCK, cols), f32),
        in_specs=[SMEM, VMEM, VMEM, SMEM],
        out_specs=VMEM,
        cost_estimate=pl.CostEstimate(flops=10**7, bytes_accessed=10**6, transcendentals=0),
    )(table, shr, up_all, y[None])

    def mine(q, t):
        return lax.dynamic_index_in_dim(bufs[q], t % slices, 0, keepdims=False)

    m = n // 2
    dn, up = [], []
    for q in range(CHUNKS):
        far = mine(q, y + half)
        dn.append(shift_slices(far[:m], slices, -1))
        up.append(shift_slices(far[m:], slices, 1))
    ends = []
    for h in range(half - 1, 0, -1):
        for q in range(CHUNKS):
            d = mine(q, y + slices - h).astype(f32)
            u = mine(q, y + h).astype(f32)
            if h == half - 1:
                d = jnp.concatenate([d[:m] + dn[q].astype(f32), d[m:]], axis=0)
                u = jnp.concatenate([u[:m], u[m:] + up[q].astype(f32)], axis=0)
            else:
                d = d + dn[q].astype(f32)
                u = u + up[q].astype(f32)
            d, u = d.astype(bf16), u.astype(bf16)
            if h > 1:
                dn[q] = shift_slices(d, slices, -1)
                up[q] = shift_slices(u, slices, 1)
            else:
                last = mine(q, y)
                oth = swap_cores(last[:, cols:], chips)
                ends += [
                    last[:, :cols],
                    shift_slices(d[:, :cols], slices, -1),
                    shift_slices(u[:, :cols], slices, 1),
                    oth,
                    shift_slices_swap(d[:, cols:], owners, slices, -1),
                    shift_slices_swap(u[:, cols:], owners, slices, 1),
                ]
    return pl.pallas_call(
        functools.partial(finish_kernel, CHUNKS),
        out_shape=jax.ShapeDtypeStruct((CORES * rows, cols), bf16),
        in_specs=[SMEM] + [VMEM] * (1 + 6 * CHUNKS),
        out_specs=VMEM,
        cost_estimate=pl.CostEstimate(flops=10**7, bytes_accessed=10**6, transcendentals=0),
    )(c[None], extra, *ends)


def solution(mesh):
    placed = (
        P(("groups", "adapter"), "tensor"),
        P("tensor", "adapter"),
        P("adapter", None, "tensor"),
        P("adapter", None, None),
        P("groups"),
        P("groups"),
        P("groups"),
    )
    return jax.shard_map(
        on_device,
        mesh=mesh,
        in_specs=placed,
        out_specs=P(("groups", "tensor"), "adapter"),
        check_vma=False,
    )
```

```python
import functools

import jax
import jax.numpy as jnp
from jax import lax
from jax.experimental import pallas as pl
from jax.experimental.pallas import tpu as pltpu
from jax.sharding import PartitionSpec as P


BLOCK = 128
CORES = 2
CHUNKS = 1
STREAMS = 1

adapter_scale = 2.0


bf16 = jnp.bfloat16
f32 = jnp.float32
i32 = jnp.int32
VMEM = pl.BlockSpec(memory_space=pltpu.VMEM)
SMEM = pl.BlockSpec(memory_space=pltpu.SMEM)
ANY = pl.BlockSpec(memory_space=pl.ANY)


def shift_chips(v, chips, step):
    pairs = [
        (x * CORES + c, ((x + step) % chips) * CORES + c)
        for x in range(chips)
        for c in range(CORES)
    ]
    return lax.ppermute(v, "adapter", pairs)


def swap_cores(v, chips):
    return lax.ppermute(v, "adapter", [(i, i ^ 1) for i in range(chips * CORES)])


def shift_slices(v, slices, step):
    return lax.ppermute(v, "tensor", [(y, (y + step) % slices) for y in range(slices)])


def shift_slices_swap(v, adapters, slices, step):
    pairs = [
        (a * slices + y, (a ^ 1) * slices + (y + step) % slices)
        for a in range(adapters)
        for y in range(slices)
    ]
    return lax.ppermute(v, ("adapter", "tensor"), pairs)


def plan_kernel(
    owners, slices, seats, where, ids, live, index, down, up,
    table, down_out, up_out, counts, seat_slot, sems
):
    slots = down.shape[0]
    rank = down.shape[1]
    blocks = ids.shape[0]
    a, y = where[0], where[1]
    c = lax.rem(a, CORES)
    for i in range(owners):
        counts[i] = 0
    for s in range(seats):
        seat_slot[s] = 0

    def block(k, _):
        slot = index[ids[k]]
        owner = lax.div(slot, slots)
        local = slot - owner * slots
        seat = jnp.minimum(counts[owner], seats - 1)
        counts[owner] = seat + 1
        table[0, k] = owner
        table[1, k] = seat
        table[2, k] = jnp.where(
            owner == a, seat, jnp.where(lax.div(owner, CORES) == lax.div(a, CORES), seats + seat, -1)
        )
        table[3, k] = live[k]

        @pl.when(owner == a)
        def _():
            seat_slot[seat] = local

        return 0

    lax.fori_loop(0, blocks, block, 0)
    cols = up.shape[2] // owners
    parts = slices // seats
    part = cols // parts
    copies = []
    for s in range(seats):
        copies.append(
            pltpu.make_async_copy(
                down.at[seat_slot[s]], down_out.at[pl.ds(s * rank, rank)], sems.at[s]
            )
        )
    up_slot = seat_slot[lax.div(y, parts)]
    low = lax.rem(y, parts) * part
    for d in range(owners):
        copies.append(
            pltpu.make_async_copy(
                up.at[up_slot, :, pl.ds(pl.multiple_of(d * cols + low, part), part)],
                up_out.at[d],
                sems.at[seats + d],
            )
        )
    for copy in copies:
        copy.start()
    for copy in copies:
        copy.wait()


def pick_kernel(rank, blk_dev, table, c_ref, shr, out):
    chips, _, _ = shr.shape
    lane = lax.broadcasted_iota(i32, (rank, BLOCK), 1)
    c = c_ref[0]
    for src in range(chips):
        for j in range(blk_dev):
            k = (src * CORES + c) * blk_dev + j
            seat = table[2, k]
            at = pl.multiple_of(jnp.maximum(seat, 0) * rank, rank)
            v = shr[src, pl.ds(at, rank), j * BLOCK : (j + 1) * BLOCK]
            live = jnp.where(seat < 0, 0, table[3, k])
            v = jnp.where(lane < live, v.astype(f32), 0.0)
            out[src, :, j * BLOCK : (j + 1) * BLOCK] = v.astype(bf16)


def extra_kernel(blk_dev, table, shr, up, y_ref, out):
    owners, rank, rows = shr.shape
    _, blk_chip, _, part = up.shape
    cols = out.shape[1]
    parts = cols // part
    y = y_ref[0]
    total = [jnp.zeros((rank, rows), f32) for _ in range(CORES)]
    for o in range(owners):
        total[o % CORES] = total[o % CORES] + shr[o].astype(f32)
    for b in range(blk_chip):
        j = b % blk_dev
        s = total[b // blk_dev][:, j * BLOCK : (j + 1) * BLOCK].astype(bf16)
        seat = table[1, y * blk_chip + b]
        for h in range(parts):
            u = up[seat * parts + h, b]
            e = lax.dot_general(s, u, (((0,), (0,)), ((), ())), preferred_element_type=f32)
            out[b * BLOCK : (b + 1) * BLOCK, h * part : (h + 1) * part] = adapter_scale * e


def on_device(
    tokens,
    query_weight,
    adapter_down_weight,
    adapter_up_weight,
    block_adapter_ids,
    block_live_count,
    adapter_slot_index,
):
    owners = lax.axis_size("adapter")
    slices = lax.axis_size("tensor")
    chips = owners // CORES
    half = chips // 2
    a = lax.axis_index("adapter")
    y = lax.axis_index("tensor")
    x, c = a // CORES, a % CORES
    rows, feats = tokens.shape
    cols = query_weight.shape[1]
    _, rank, _ = adapter_up_weight.shape
    blocks = block_adapter_ids.shape[0]
    seats = 2 * blocks // owners
    blk_dev = blocks // owners
    blk_chip = blk_dev * CORES
    parts = slices // seats
    part = cols // parts
    n = rows // CHUNKS

    chunks = [tokens[q * n : (q + 1) * n] for q in range(CHUNKS)]
    ups, dns = [], []
    for q in range(CHUNKS):
        ups.append([shift_chips(chunks[q], chips, 1)])
        dns.append([shift_chips(chunks[q], chips, -1)])
    w_oth = swap_cores(query_weight, chips)
    w_both = jnp.concatenate([query_weight, w_oth], axis=1)

    table, down_own, up_part = pl.pallas_call(
        functools.partial(plan_kernel, owners, slices, seats),
        out_shape=(
            jax.ShapeDtypeStruct((4, blocks), i32),
            jax.ShapeDtypeStruct((seats * rank, feats), bf16),
            jax.ShapeDtypeStruct((owners, rank, part), bf16),
        ),
        in_specs=[SMEM] * 4 + [ANY] * 2,
        out_specs=(SMEM, VMEM, VMEM),
        scratch_shapes=[
            pltpu.SMEM((owners,), i32),
            pltpu.SMEM((seats,), i32),
            pltpu.SemaphoreType.DMA((seats + owners,)),
        ],
        cost_estimate=pl.CostEstimate(flops=10**7, bytes_accessed=10**6, transcendentals=0),
    )(
        jnp.stack([a, y]),
        block_adapter_ids,
        block_live_count,
        adapter_slot_index,
        adapter_down_weight,
        adapter_up_weight,
    )
    down_oth = swap_cores(down_own, chips)
    down_chip = jnp.concatenate([down_own, down_oth], axis=0)
    up_part = lax.all_to_all(up_part, "adapter", 0, 0, tiled=True)
    up_all = jnp.take(up_part, table[0], axis=0).reshape(slices, blk_chip, rank, part)
    up_all = lax.all_to_all(up_all, "tensor", 0, 0, tiled=True)

    shr_buf = jnp.zeros((chips, CORES * seats * rank, rows), bf16)
    bufs = []

    def put(q, tok, d):
        nonlocal shr_buf
        src = (x + d) % chips
        p = jnp.dot(tok, w_both, preferred_element_type=f32).astype(bf16)
        bufs[q] = lax.dynamic_update_slice(bufs[q], p[None], (src, 0, 0))
        s = lax.dot_general(
            down_chip, tok, (((1,), (1,)), ((), ())), preferred_element_type=f32
        ).astype(bf16)
        shr_buf = lax.dynamic_update_slice(shr_buf, s[None], (src, 0, q * n))

    for q in range(CHUNKS):
        bufs.append(jnp.zeros((chips, n, CORES * cols), bf16))
        put(q, chunks[q], 0)
    for h in range(1, half + 1):
        for q in range(CHUNKS):
            if h == half:
                tok = jnp.concatenate([ups[q][-1], dns[q][-1]], axis=0)
                put(q, tok, half)
                continue
            put(q, ups[q][-1], -h)
            put(q, dns[q][-1], h)
            up, dn = ups[q][-1], dns[q][-1]
            if h == half - 1:
                up, dn = up[: n // 2], dn[n // 2 :]
            ups[q].append(shift_chips(up, chips, 1))
            dns[q].append(shift_chips(dn, chips, -1))

    pick = pl.pallas_call(
        functools.partial(pick_kernel, rank, blk_dev),
        name="pick",
        out_shape=jax.ShapeDtypeStruct((chips, rank, rows), bf16),
        in_specs=[SMEM, SMEM, VMEM],
        out_specs=VMEM,
        cost_estimate=pl.CostEstimate(flops=10**7, bytes_accessed=10**6, transcendentals=0),
    )
    shr = pick(table, c[None], shr_buf)
    shr, up_all = lax.optimization_barrier((shr, up_all))
    shr = lax.all_to_all(shr, "tensor", 0, 0, tiled=True)
    shr = jnp.sum(shr.astype(f32), axis=0).astype(bf16)
    shr = jnp.broadcast_to(shr[None], (owners, rank, rows))
    shr = lax.all_to_all(shr, "adapter", 0, 0, tiled=True)
    expand = pl.pallas_call(
        functools.partial(extra_kernel, blk_dev),
        name="extra",
        out_shape=jax.ShapeDtypeStruct((blk_chip * BLOCK, cols), f32),
        in_specs=[SMEM, VMEM, VMEM, SMEM],
        out_specs=VMEM,
        cost_estimate=pl.CostEstimate(flops=10**7, bytes_accessed=10**6, transcendentals=0),
    )
    extra = expand(table, shr, up_all, y[None])

    k = rows // STREAMS
    m = k // 2

    def mine(t, lo, size):
        return lax.dynamic_slice(bufs[0], (t % slices, lo, 0), (1, size, CORES * cols))[0]

    dn, up, ends = [], [], []
    for r in range(STREAMS):
        dn.append(shift_slices(mine(y + half, r * k, m), slices, -1))
        up.append(shift_slices(mine(y + half, r * k + m, m), slices, 1))
    last = mine(y, 0, rows)
    oth = swap_cores(last[:, cols:], chips)
    before = None
    for h in range(half - 1, 0, -1):
        for r in range(STREAMS):
            if before is None:
                dn[r], up[r] = lax.optimization_barrier((dn[r], up[r]))
            else:
                dn[r], up[r], before = lax.optimization_barrier((dn[r], up[r], before))
            d = mine(y + slices - h, r * k, k).astype(f32)
            u = mine(y + h, r * k, k).astype(f32)
            if h == half - 1:
                d = jnp.concatenate([d[:m] + dn[r].astype(f32), d[m:]], axis=0)
                u = jnp.concatenate([u[:m], u[m:] + up[r].astype(f32)], axis=0)
            else:
                d = d + dn[r].astype(f32)
                u = u + up[r].astype(f32)
            d, u = d.astype(bf16), u.astype(bf16)
            if h == 1:
                d, dx = d[:, :cols], d[:, cols:]
                u, ux = u[:, :cols], u[:, cols:]
            before = d
            dn[r] = shift_slices(d, slices, -1)
            up[r] = shift_slices(u, slices, 1)
            if h == 1:
                dx = shift_slices_swap(dx, owners, slices, -1)
                ux = shift_slices_swap(ux, owners, slices, 1)
                ends += [dn[r], up[r], dx, ux]
    out = []
    order = lax.broadcasted_iota(i32, (CORES, k, cols), 0)
    extra = extra.reshape(CORES, rows, cols)
    for r in range(STREAMS):
        sums = [v.astype(f32)[None] for v in ends[4 * r : 4 * r + 4]]
        v_own = last[r * k : (r + 1) * k, :cols].astype(f32)[None] + sums[0] + sums[1]
        v_oth = oth[r * k : (r + 1) * k].astype(f32)[None] + sums[2] + sums[3]
        v = jnp.where(order == c, v_own, v_oth) + extra[:, r * k : (r + 1) * k]
        out.append(v.astype(bf16))
    return jnp.concatenate(out, axis=1).reshape(CORES * rows, cols)


def solution(mesh):
    placed = (
        P(("groups", "adapter"), "tensor"),
        P("tensor", "adapter"),
        P("adapter", None, "tensor"),
        P("adapter", None, None),
        P("groups"),
        P("groups"),
        P("groups"),
    )
    return jax.shard_map(
        on_device,
        mesh=mesh,
        in_specs=placed,
        out_specs=P(("groups", "tensor"), "adapter"),
        check_vma=False,
    )
```

```python
import functools

import jax
import jax.numpy as jnp
from jax import lax
from jax.experimental import pallas as pl
from jax.experimental.pallas import tpu as pltpu
from jax.sharding import PartitionSpec as P


BLOCK = 128
CORES = 2
CHUNKS = 1
STREAMS = 1

adapter_scale = 2.0


bf16 = jnp.bfloat16
f32 = jnp.float32
i32 = jnp.int32
VMEM = pl.BlockSpec(memory_space=pltpu.VMEM)
SMEM = pl.BlockSpec(memory_space=pltpu.SMEM)
ANY = pl.BlockSpec(memory_space=pl.ANY)


def shift_chips(v, chips, step):
    pairs = [
        (x * CORES + c, ((x + step) % chips) * CORES + c)
        for x in range(chips)
        for c in range(CORES)
    ]
    return lax.ppermute(v, "adapter", pairs)


def swap_cores(v, chips):
    return lax.ppermute(v, "adapter", [(i, i ^ 1) for i in range(chips * CORES)])


def shift_slices(v, slices, step):
    return lax.ppermute(v, "tensor", [(y, (y + step) % slices) for y in range(slices)])


def shift_slices_swap(v, adapters, slices, step):
    pairs = [
        (a * slices + y, (a ^ 1) * slices + (y + step) % slices)
        for a in range(adapters)
        for y in range(slices)
    ]
    return lax.ppermute(v, ("adapter", "tensor"), pairs)


def plan_kernel(
    owners, slices, seats, where, ids, live, index, down, up,
    table, down_out, up_out, counts, seat_slot, sems
):
    slots = down.shape[0]
    rank = down.shape[1]
    blocks = ids.shape[0]
    a, y = where[0], where[1]
    c = lax.rem(a, CORES)
    for i in range(owners):
        counts[i] = 0
    for s in range(seats):
        seat_slot[s] = 0

    def block(k, _):
        slot = index[ids[k]]
        owner = lax.div(slot, slots)
        local = slot - owner * slots
        seat = jnp.minimum(counts[owner], seats - 1)
        counts[owner] = seat + 1
        table[0, k] = owner
        table[1, k] = seat
        table[2, k] = jnp.where(
            owner == a, seat, jnp.where(lax.div(owner, CORES) == lax.div(a, CORES), seats + seat, -1)
        )
        table[3, k] = live[k]

        @pl.when(owner == a)
        def _():
            seat_slot[seat] = local

        return 0

    lax.fori_loop(0, blocks, block, 0)
    cols = up.shape[2] // owners
    parts = slices // seats
    part = cols // parts
    copies = []
    for s in range(seats):
        copies.append(
            pltpu.make_async_copy(
                down.at[seat_slot[s]], down_out.at[pl.ds(s * rank, rank)], sems.at[s]
            )
        )
    up_slot = seat_slot[lax.div(y, parts)]
    low = lax.rem(y, parts) * part
    for d in range(owners):
        copies.append(
            pltpu.make_async_copy(
                up.at[up_slot, :, pl.ds(pl.multiple_of(d * cols + low, part), part)],
                up_out.at[d],
                sems.at[seats + d],
            )
        )
    for copy in copies:
        copy.start()
    for copy in copies:
        copy.wait()


def pick_kernel(rank, blk_dev, table, c_ref, shr, out):
    chips, _, _ = shr.shape
    lane = lax.broadcasted_iota(i32, (rank, BLOCK), 1)
    c = c_ref[0]
    for src in range(chips):
        for j in range(blk_dev):
            k = (src * CORES + c) * blk_dev + j
            seat = table[2, k]
            at = pl.multiple_of(jnp.maximum(seat, 0) * rank, rank)
            v = shr[src, pl.ds(at, rank), j * BLOCK : (j + 1) * BLOCK]
            live = jnp.where(seat < 0, 0, table[3, k])
            v = jnp.where(lane < live, v.astype(f32), 0.0)
            out[src, :, j * BLOCK : (j + 1) * BLOCK] = v.astype(bf16)


def extra_kernel(blk_dev, table, shr, up, y_ref, out):
    owners, rank, rows = shr.shape
    _, blk_chip, _, part = up.shape
    cols = out.shape[1]
    parts = cols // part
    y = y_ref[0]
    total = [jnp.zeros((rank, rows), f32) for _ in range(CORES)]
    for o in range(owners):
        total[o % CORES] = total[o % CORES] + shr[o].astype(f32)
    for b in range(blk_chip):
        j = b % blk_dev
        s = total[b // blk_dev][:, j * BLOCK : (j + 1) * BLOCK].astype(bf16)
        seat = table[1, y * blk_chip + b]
        for h in range(parts):
            u = up[seat * parts + h, b]
            e = lax.dot_general(s, u, (((0,), (0,)), ((), ())), preferred_element_type=f32)
            out[b * BLOCK : (b + 1) * BLOCK, h * part : (h + 1) * part] = adapter_scale * e


def on_device(
    tokens,
    query_weight,
    adapter_down_weight,
    adapter_up_weight,
    block_adapter_ids,
    block_live_count,
    adapter_slot_index,
):
    owners = lax.axis_size("adapter")
    slices = lax.axis_size("tensor")
    chips = owners // CORES
    half = chips // 2
    a = lax.axis_index("adapter")
    y = lax.axis_index("tensor")
    x, c = a // CORES, a % CORES
    rows, feats = tokens.shape
    cols = query_weight.shape[1]
    _, rank, _ = adapter_up_weight.shape
    blocks = block_adapter_ids.shape[0]
    seats = 2 * blocks // owners
    blk_dev = blocks // owners
    blk_chip = blk_dev * CORES
    parts = slices // seats
    part = cols // parts
    n = rows // CHUNKS

    chunks = [tokens[q * n : (q + 1) * n] for q in range(CHUNKS)]
    ups, dns = [], []
    for q in range(CHUNKS):
        ups.append([shift_chips(chunks[q], chips, 1)])
        dns.append([shift_chips(chunks[q], chips, -1)])
    w_oth = swap_cores(query_weight, chips)
    w_both = jnp.concatenate([query_weight, w_oth], axis=1)

    table, down_own, up_part = pl.pallas_call(
        functools.partial(plan_kernel, owners, slices, seats),
        out_shape=(
            jax.ShapeDtypeStruct((4, blocks), i32),
            jax.ShapeDtypeStruct((seats * rank, feats), bf16),
            jax.ShapeDtypeStruct((owners, rank, part), bf16),
        ),
        in_specs=[SMEM] * 4 + [ANY] * 2,
        out_specs=(SMEM, VMEM, VMEM),
        scratch_shapes=[
            pltpu.SMEM((owners,), i32),
            pltpu.SMEM((seats,), i32),
            pltpu.SemaphoreType.DMA((seats + owners,)),
        ],
        cost_estimate=pl.CostEstimate(flops=10**7, bytes_accessed=10**6, transcendentals=0),
    )(
        jnp.stack([a, y]),
        block_adapter_ids,
        block_live_count,
        adapter_slot_index,
        adapter_down_weight,
        adapter_up_weight,
    )
    down_oth = swap_cores(down_own, chips)
    down_chip = jnp.concatenate([down_own, down_oth], axis=0)
    up_part = lax.all_to_all(up_part, "adapter", 0, 0, tiled=True)
    up_all = jnp.take(up_part, table[0], axis=0).reshape(slices, blk_chip, rank, part)
    up_all = lax.all_to_all(up_all, "tensor", 0, 0, tiled=True)

    shr_buf = jnp.zeros((chips, CORES * seats * rank, rows), bf16)
    bufs = []

    def put(q, tok, d):
        nonlocal shr_buf
        src = (x + d) % chips
        p = jnp.dot(tok, w_both, preferred_element_type=f32).astype(bf16)
        bufs[q] = lax.dynamic_update_slice(bufs[q], p[None], ((src - y) % slices, 0, 0))
        s = lax.dot_general(
            down_chip, tok, (((1,), (1,)), ((), ())), preferred_element_type=f32
        ).astype(bf16)
        shr_buf = lax.dynamic_update_slice(shr_buf, s[None], (src, 0, q * n))

    for q in range(CHUNKS):
        bufs.append(jnp.zeros((chips, n, CORES * cols), bf16))
        put(q, chunks[q], 0)
    for h in range(1, half + 1):
        for q in range(CHUNKS):
            if h == half:
                tok = jnp.concatenate([ups[q][-1], dns[q][-1]], axis=0)
                put(q, tok, half)
                continue
            put(q, ups[q][-1], -h)
            put(q, dns[q][-1], h)
            up, dn = ups[q][-1], dns[q][-1]
            if h == half - 1:
                up, dn = up[: n // 2], dn[n // 2 :]
            ups[q].append(shift_chips(up, chips, 1))
            dns[q].append(shift_chips(dn, chips, -1))

    pick = pl.pallas_call(
        functools.partial(pick_kernel, rank, blk_dev),
        name="pick",
        out_shape=jax.ShapeDtypeStruct((chips, rank, rows), bf16),
        in_specs=[SMEM, SMEM, VMEM],
        out_specs=VMEM,
        cost_estimate=pl.CostEstimate(flops=10**7, bytes_accessed=10**6, transcendentals=0),
        compiler_params=pltpu.CompilerParams(vmem_limit_bytes=6 * 2**20),
    )
    shr = pick(table, c[None], shr_buf)
    shr, up_all = lax.optimization_barrier((shr, up_all))
    shr = lax.all_to_all(shr, "tensor", 0, 0, tiled=True)
    shr = jnp.sum(shr.astype(f32), axis=0).astype(bf16)
    shr = jnp.broadcast_to(shr[None], (owners, rank, rows))
    shr = lax.all_to_all(shr, "adapter", 0, 0, tiled=True)
    expand = pl.pallas_call(
        functools.partial(extra_kernel, blk_dev),
        name="extra",
        out_shape=jax.ShapeDtypeStruct((blk_chip * BLOCK, cols), f32),
        in_specs=[SMEM, VMEM, VMEM, SMEM],
        out_specs=VMEM,
        cost_estimate=pl.CostEstimate(flops=10**7, bytes_accessed=10**6, transcendentals=0),
        compiler_params=pltpu.CompilerParams(vmem_limit_bytes=6 * 2**20),
    )
    extra = expand(table, shr, up_all, y[None])

    k = rows // STREAMS
    m = k // 2

    def mine(t, lo, size):
        return bufs[0][t % slices, lo : lo + size]

    dn, up, ends = [], [], []
    for r in range(STREAMS):
        dn.append(shift_slices(mine(half, r * k, m), slices, -1))
        up.append(shift_slices(mine(half, r * k + m, m), slices, 1))
    last = mine(0, 0, rows)
    oth = swap_cores(last[:, cols:], chips)
    before = None
    for h in range(half - 1, 0, -1):
        for r in range(STREAMS):
            if before is None:
                dn[r], up[r] = lax.optimization_barrier((dn[r], up[r]))
            else:
                dn[r], up[r], before = lax.optimization_barrier((dn[r], up[r], before))
            d = mine(slices - h, r * k, k).astype(f32)
            u = mine(h, r * k, k).astype(f32)
            if h == half - 1:
                d = jnp.concatenate([d[:m] + dn[r].astype(f32), d[m:]], axis=0)
                u = jnp.concatenate([u[:m], u[m:] + up[r].astype(f32)], axis=0)
            else:
                d = d + dn[r].astype(f32)
                u = u + up[r].astype(f32)
            d, u = d.astype(bf16), u.astype(bf16)
            if h == 1:
                d, dx = d[:, :cols], d[:, cols:]
                u, ux = u[:, :cols], u[:, cols:]
            before = d
            dn[r] = shift_slices(d, slices, -1)
            up[r] = shift_slices(u, slices, 1)
            if h == 1:
                dx = shift_slices_swap(dx, owners, slices, -1)
                ux = shift_slices_swap(ux, owners, slices, 1)
                ends += [dn[r], up[r], dx, ux]
    out = []
    order = lax.broadcasted_iota(i32, (CORES, k, cols), 0)
    extra = extra.reshape(CORES, rows, cols)
    for r in range(STREAMS):
        sums = [v.astype(f32)[None] for v in ends[4 * r : 4 * r + 4]]
        v_own = last[r * k : (r + 1) * k, :cols].astype(f32)[None] + sums[0] + sums[1]
        v_oth = oth[r * k : (r + 1) * k].astype(f32)[None] + sums[2] + sums[3]
        v = jnp.where(order == c, v_own, v_oth) + extra[:, r * k : (r + 1) * k]
        out.append(v.astype(bf16))
    return jnp.concatenate(out, axis=1).reshape(CORES * rows, cols)


def solution(mesh):
    placed = (
        P(("groups", "adapter"), "tensor"),
        P("tensor", "adapter"),
        P("adapter", None, "tensor"),
        P("adapter", None, None),
        P("groups"),
        P("groups"),
        P("groups"),
    )
    return jax.shard_map(
        on_device,
        mesh=mesh,
        in_specs=placed,
        out_specs=P(("groups", "tensor"), "adapter"),
        check_vma=False,
    )
```

```python
import functools

import jax
import jax.numpy as jnp
from jax import lax
from jax.experimental import pallas as pl
from jax.experimental.layout import Layout, with_layout_constraint
from jax.experimental.pallas import tpu as pltpu
from jax.sharding import PartitionSpec as P


BLOCK = 128
CORES = 2
CHUNKS = 1
STREAMS = 1

adapter_scale = 2.0


bf16 = jnp.bfloat16
f32 = jnp.float32
i32 = jnp.int32
VMEM = pl.BlockSpec(memory_space=pltpu.VMEM)
SMEM = pl.BlockSpec(memory_space=pltpu.SMEM)
ANY = pl.BlockSpec(memory_space=pl.ANY)


def shift_chips(v, chips, step):
    pairs = [
        (x * CORES + c, ((x + step) % chips) * CORES + c)
        for x in range(chips)
        for c in range(CORES)
    ]
    return lax.ppermute(v, "adapter", pairs)


def swap_cores(v, chips):
    return lax.ppermute(v, "adapter", [(i, i ^ 1) for i in range(chips * CORES)])


def shift_slices(v, slices, step):
    return lax.ppermute(v, "tensor", [(y, (y + step) % slices) for y in range(slices)])


def shift_slices_swap(v, adapters, slices, step):
    pairs = [
        (a * slices + y, (a ^ 1) * slices + (y + step) % slices)
        for a in range(adapters)
        for y in range(slices)
    ]
    return lax.ppermute(v, ("adapter", "tensor"), pairs)


def plan_kernel(
    owners, slices, seats, where, ids, live, index, down, up,
    table, down_out, up_out, counts, seat_slot, sems
):
    slots = down.shape[0]
    rank = down.shape[1]
    blocks = ids.shape[0]
    a, y = where[0], where[1]
    c = lax.rem(a, CORES)
    for i in range(owners):
        counts[i] = 0
    for s in range(seats):
        seat_slot[s] = 0

    def block(k, _):
        slot = index[ids[k]]
        owner = lax.div(slot, slots)
        local = slot - owner * slots
        seat = jnp.minimum(counts[owner], seats - 1)
        counts[owner] = seat + 1
        table[0, k] = owner
        table[1, k] = seat
        table[2, k] = jnp.where(
            owner == a, seat, jnp.where(lax.div(owner, CORES) == lax.div(a, CORES), seats + seat, -1)
        )
        table[3, k] = live[k]

        @pl.when(owner == a)
        def _():
            seat_slot[seat] = local

        return 0

    lax.fori_loop(0, blocks, block, 0)
    cols = up.shape[2] // owners
    parts = slices // seats
    part = cols // parts
    copies = []
    for s in range(seats):
        copies.append(
            pltpu.make_async_copy(
                down.at[seat_slot[s]], down_out.at[pl.ds(s * rank, rank)], sems.at[s]
            )
        )
    up_slot = seat_slot[lax.div(y, parts)]
    low = lax.rem(y, parts) * part
    for d in range(owners):
        copies.append(
            pltpu.make_async_copy(
                up.at[up_slot, :, pl.ds(pl.multiple_of(d * cols + low, part), part)],
                up_out.at[d],
                sems.at[seats + d],
            )
        )
    for copy in copies:
        copy.start()
    for copy in copies:
        copy.wait()


def pick_kernel(rank, blk_dev, table, c_ref, shr, out):
    chips, _, _ = shr.shape
    lane = lax.broadcasted_iota(i32, (rank, BLOCK), 1)
    c = c_ref[0]
    for src in range(chips):
        for j in range(blk_dev):
            k = (src * CORES + c) * blk_dev + j
            seat = table[2, k]
            at = pl.multiple_of(jnp.maximum(seat, 0) * rank, rank)
            v = shr[src, pl.ds(at, rank), j * BLOCK : (j + 1) * BLOCK]
            live = jnp.where(seat < 0, 0, table[3, k])
            v = jnp.where(lane < live, v.astype(f32), 0.0)
            out[src, :, j * BLOCK : (j + 1) * BLOCK] = v.astype(bf16)


def extra_kernel(blk_dev, table, shr, up, y_ref, out):
    owners, rank, rows = shr.shape
    _, blk_chip, _, part = up.shape
    cols = out.shape[1]
    parts = cols // part
    y = y_ref[0]
    total = [jnp.zeros((rank, rows), f32) for _ in range(CORES)]
    for o in range(owners):
        total[o % CORES] = total[o % CORES] + shr[o].astype(f32)
    for b in range(blk_chip):
        j = b % blk_dev
        s = total[b // blk_dev][:, j * BLOCK : (j + 1) * BLOCK].astype(bf16)
        seat = table[1, y * blk_chip + b]
        for h in range(parts):
            u = up[seat * parts + h, b]
            e = lax.dot_general(s, u, (((0,), (0,)), ((), ())), preferred_element_type=f32)
            out[b * BLOCK : (b + 1) * BLOCK, h * part : (h + 1) * part] = adapter_scale * e


def on_device(
    tokens,
    query_weight,
    adapter_down_weight,
    adapter_up_weight,
    block_adapter_ids,
    block_live_count,
    adapter_slot_index,
):
    owners = lax.axis_size("adapter")
    slices = lax.axis_size("tensor")
    chips = owners // CORES
    half = chips // 2
    a = lax.axis_index("adapter")
    y = lax.axis_index("tensor")
    x, c = a // CORES, a % CORES
    rows, feats = tokens.shape
    cols = query_weight.shape[1]
    _, rank, _ = adapter_up_weight.shape
    blocks = block_adapter_ids.shape[0]
    seats = 2 * blocks // owners
    blk_dev = blocks // owners
    blk_chip = blk_dev * CORES
    parts = slices // seats
    part = cols // parts
    n = rows // CHUNKS

    chunks = [tokens[q * n : (q + 1) * n] for q in range(CHUNKS)]
    ups, dns = [], []
    for q in range(CHUNKS):
        ups.append([shift_chips(chunks[q], chips, 1)])
        dns.append([shift_chips(chunks[q], chips, -1)])
    w_oth = swap_cores(query_weight, chips)
    w_both = jnp.concatenate([query_weight, w_oth], axis=1)

    table, down_own, up_part = pl.pallas_call(
        functools.partial(plan_kernel, owners, slices, seats),
        out_shape=(
            jax.ShapeDtypeStruct((4, blocks), i32),
            jax.ShapeDtypeStruct((seats * rank, feats), bf16),
            jax.ShapeDtypeStruct((owners, rank, part), bf16),
        ),
        in_specs=[SMEM] * 4 + [ANY] * 2,
        out_specs=(SMEM, VMEM, VMEM),
        scratch_shapes=[
            pltpu.SMEM((owners,), i32),
            pltpu.SMEM((seats,), i32),
            pltpu.SemaphoreType.DMA((seats + owners,)),
        ],
        cost_estimate=pl.CostEstimate(flops=10**7, bytes_accessed=10**6, transcendentals=0),
    )(
        jnp.stack([a, y]),
        block_adapter_ids,
        block_live_count,
        adapter_slot_index,
        adapter_down_weight,
        adapter_up_weight,
    )
    down_oth = swap_cores(down_own, chips)
    down_chip = jnp.concatenate([down_own, down_oth], axis=0)
    up_part = lax.all_to_all(up_part, "adapter", 0, 0, tiled=True)
    up_all = jnp.take(up_part, table[0], axis=0).reshape(slices, blk_chip, rank, part)
    up_all = lax.all_to_all(up_all, "tensor", 0, 0, tiled=True)

    shr_buf = jnp.zeros((chips, CORES * seats * rank, rows), bf16)
    bufs = []

    def put(q, tok, d):
        nonlocal shr_buf
        src = (x + d) % chips
        p = jnp.dot(tok, w_both, preferred_element_type=f32).astype(bf16)
        p = with_layout_constraint(p, Layout((0, 1)))
        bufs[q] = lax.dynamic_update_slice(bufs[q], p[None], ((src - y) % slices, 0, 0))
        s = lax.dot_general(
            down_chip, tok, (((1,), (1,)), ((), ())), preferred_element_type=f32
        ).astype(bf16)
        shr_buf = lax.dynamic_update_slice(shr_buf, s[None], (src, 0, q * n))

    for q in range(CHUNKS):
        bufs.append(jnp.zeros((chips, n, CORES * cols), bf16))
        put(q, chunks[q], 0)
    for h in range(1, half + 1):
        for q in range(CHUNKS):
            if h == half:
                tok = jnp.concatenate([ups[q][-1], dns[q][-1]], axis=0)
                put(q, tok, half)
                continue
            put(q, ups[q][-1], -h)
            put(q, dns[q][-1], h)
            up, dn = ups[q][-1], dns[q][-1]
            if h == half - 1:
                up, dn = up[: n // 2], dn[n // 2 :]
            ups[q].append(shift_chips(up, chips, 1))
            dns[q].append(shift_chips(dn, chips, -1))

    pick = pl.pallas_call(
        functools.partial(pick_kernel, rank, blk_dev),
        name="pick",
        out_shape=jax.ShapeDtypeStruct((chips, rank, rows), bf16),
        in_specs=[SMEM, SMEM, VMEM],
        out_specs=VMEM,
        cost_estimate=pl.CostEstimate(flops=10**7, bytes_accessed=10**6, transcendentals=0),
        compiler_params=pltpu.CompilerParams(vmem_limit_bytes=6 * 2**20),
    )
    shr = pick(table, c[None], shr_buf)
    shr, up_all = lax.optimization_barrier((shr, up_all))
    shr = lax.all_to_all(shr, "tensor", 0, 0, tiled=True)
    shr = jnp.sum(shr.astype(f32), axis=0).astype(bf16)
    shr = jnp.broadcast_to(shr[None], (owners, rank, rows))
    shr = lax.all_to_all(shr, "adapter", 0, 0, tiled=True)
    expand = pl.pallas_call(
        functools.partial(extra_kernel, blk_dev),
        name="extra",
        out_shape=jax.ShapeDtypeStruct((blk_chip * BLOCK, cols), f32),
        in_specs=[SMEM, VMEM, VMEM, SMEM],
        out_specs=VMEM,
        cost_estimate=pl.CostEstimate(flops=10**7, bytes_accessed=10**6, transcendentals=0),
        compiler_params=pltpu.CompilerParams(vmem_limit_bytes=6 * 2**20),
    )
    extra = expand(table, shr, up_all, y[None])

    k = rows // STREAMS
    m = k // 2

    def mine(t, lo, size):
        return bufs[0][t % slices, lo : lo + size]

    h = half - 1
    dn = shift_slices(mine(half, 0, m), slices, -1)
    up = shift_slices(mine(half, m, m), slices, 1)
    dn_b = shift_slices(mine(slices - h, m, m), slices, -1)
    up_b = shift_slices(mine(h, 0, m), slices, 1)
    last = mine(0, 0, rows)
    oth = swap_cores(last[:, cols:], chips)
    dn, up = lax.optimization_barrier((dn, up))
    d = (mine(slices - h, 0, m).astype(f32) + dn.astype(f32)).astype(bf16)
    u = (mine(h, m, m).astype(f32) + up.astype(f32)).astype(bf16)
    dn = shift_slices(d, slices, -1)
    up = shift_slices(u, slices, 1)
    dn, up, dn_b, up_b = lax.optimization_barrier((dn, up, dn_b, up_b))
    dn = jnp.concatenate([dn, dn_b], axis=0)
    up = jnp.concatenate([up_b, up], axis=0)
    for h in range(half - 2, 0, -1):
        if h < half - 2:
            dn, up = lax.optimization_barrier((dn, up))
        d = (mine(slices - h, 0, rows).astype(f32) + dn.astype(f32)).astype(bf16)
        u = (mine(h, 0, rows).astype(f32) + up.astype(f32)).astype(bf16)
        if h > 1:
            dn = shift_slices(d, slices, -1)
            up = shift_slices(u, slices, 1)
        else:
            dn = shift_slices(d[:, :cols], slices, -1)
            up = shift_slices(u[:, :cols], slices, 1)
            dx = shift_slices_swap(d[:, cols:], owners, slices, -1)
            ux = shift_slices_swap(u[:, cols:], owners, slices, 1)
    ends = [dn, up, dx, ux]
    out = []
    order = lax.broadcasted_iota(i32, (CORES, k, cols), 0)
    extra = extra.reshape(CORES, rows, cols)
    for r in range(STREAMS):
        sums = [v.astype(f32)[None] for v in ends[4 * r : 4 * r + 4]]
        v_own = last[r * k : (r + 1) * k, :cols].astype(f32)[None] + sums[0] + sums[1]
        v_oth = oth[r * k : (r + 1) * k].astype(f32)[None] + sums[2] + sums[3]
        v = jnp.where(order == c, v_own, v_oth) + extra[:, r * k : (r + 1) * k]
        out.append(v.astype(bf16))
    return jnp.concatenate(out, axis=1).reshape(CORES * rows, cols)


def solution(mesh):
    placed = (
        P(("groups", "adapter"), "tensor"),
        P("tensor", "adapter"),
        P("adapter", None, "tensor"),
        P("adapter", None, None),
        P("groups"),
        P("groups"),
        P("groups"),
    )
    return jax.shard_map(
        on_device,
        mesh=mesh,
        in_specs=placed,
        out_specs=P(("groups", "tensor"), "adapter"),
        check_vma=False,
    )
```
